256 devices in a mesh: sweep: 2 (over z), expert: 16 (over y, core), fsdp: 8 (over x).
Axes of the slice: x: 8, y: 8, z: 2, core: 2. Of those that a mesh axis runs over, the one named last changes fastest.
The devices are a block of a 8x8x16 slice.
Arguments:
- tokens: bfloat16 [32768, 2048], P(('sweep', 'expert', 'fsdp')), parts along dimension 0, may hold values from -6 to 6
- context: bfloat16 [32768, 2048], P(('sweep', 'expert', 'fsdp')), parts along dimension 0, may hold values from -6 to 6
- out_proj: bfloat16 [4096, 2048], P(('sweep', 'expert', 'fsdp')), parts along dimension 0, may hold values from -0.125 to 0.125
- norm_gain: float32 [4096], P('sweep'), parts along dimension 0, may hold values from 0.1 to 1.9
- router: bfloat16 [4096, 64], P('sweep'), parts along dimension 0, may hold values from -0.125 to 0.125
- expert_ids: int32 [32768, 2], P(('sweep', 'expert', 'fsdp')), parts along dimension 0, may hold values from 0 to 63, all different within a row; in each aligned block of 128 rows (0 to 127, 128 to 255, ...) at most 5 rows name the same one
- w_gate_up: bfloat16 [256, 2, 704, 2048], P(('sweep', 'expert', 'fsdp')), parts along dimension 0, may hold values from -0.125 to 0.125
- w_down: bfloat16 [256, 704, 2048], P(('sweep', 'expert', 'fsdp')), parts along dimension 0, may hold values from -0.15625 to 0.15625
Outputs:
- layer_out: bfloat16 [32768, 2048], P(('sweep', 'expert', 'fsdp')), parts along dimension 0
The draws below stay inside these ranges and needn't reach their ends.
There are 2 independent parts, one for each index of `sweep`. The reference program is written for one: setup_inputs(seed, part) draws one part's arguments, and reference() takes and returns one part's arrays. A program takes and returns all parts, laid end to end along the dimension named above; each array names one. Nothing has to cross between parts.
Inputs may be any that keep to these rules, and one draw needn't show every extreme that they name: `expert_ids`: each row names two different experts. Among the rows of one device no expert is named more than 5 times, a bound that some block reaches.
All inputs are finite; a program needn't handle non-finite values.
Results may differ from the reference program's by a relative error of at most 0.012.
Values may be sent and summed in bfloat16 or wider, within the bound.
A program may use at most 64 MiB of HBM per device.

```python
import math
import jax
import jax.numpy as jnp
import numpy as np
from jax import lax

D = 2048
FF = 1408
EXPERTS = 64
TOK_DEV = 128
CAP = 5
TOKENS = 16384
N_EXPERT = 16
N_FSDP = 8


def block_scale(own_key, dims, cuts, least, high):
    def one(dim, blocks):
        steps = jax.random.uniform(jax.random.fold_in(jax.random.fold_in(own_key, 6), dim), (blocks,), jnp.float32, least / len(cuts), high / len(cuts))
        return jnp.repeat(jnp.exp(steps), dims[dim] // blocks).reshape((-1,) + (1,) * (len(dims) - dim - 1))

    factor_of = one(*cuts[0])
    for cut in cuts[1:]:
        factor_of = factor_of * one(*cut)
    return factor_of


def assign_block(own_key, own, number, rows, number_of, top, most, skew):
    order = jax.random.permutation(own_key, number_of)
    packed, ordinary = portions_of(number_of, rows * top, most, skew, True), portions_of(number_of, rows * top, most, skew, False)
    places = jnp.arange(number_of)

    def named(lengths, turn):
        used = int((lengths > 0).sum())
        fixed = max(1, used // 4)
        moved = fixed + (places - fixed + turn * (used - fixed)) % max(1, number_of - fixed)
        return jnp.zeros((number_of,), jnp.int32).at[order[jnp.where(places < fixed, places, moved)]].set(jnp.asarray(lengths, jnp.int32))

    lengths = jnp.where(number % 4 == 0, named(packed, number // 4), named(ordinary, number - number // 4 - 1))
    mixed = jax.random.permutation(jax.random.fold_in(own, 3), number_of)
    giver, receiver = mixed[0:number_of // 2 * 2:2], mixed[1:number_of // 2 * 2:2]
    margin = jnp.minimum(lengths[giver] - 1, most - lengths[receiver]) // 2
    margin = jnp.where((giver == order[0]) | (receiver == order[0]) | (lengths[receiver] == 0), 0, jnp.maximum(margin, 0))
    moved = jax.random.randint(jax.random.fold_in(own, 4), (number_of // 2,), 0, 1 << 20) % (margin + 1)
    lengths = lengths.at[giver].add(-moved).at[receiver].add(moved)
    items = jnp.searchsorted(jnp.cumsum(lengths), jnp.arange(rows * top), side="right").astype(jnp.int32)
    listing = items.reshape(top, rows).T
    listing = listing[jax.random.permutation(jax.random.fold_in(own, 1), rows)]
    turn = jax.random.randint(jax.random.fold_in(own, 2), (rows, 1), 0, top)
    return jnp.take_along_axis(listing, (jnp.arange(top)[None, :] + turn) % top, axis=1)


def portions_of(count, total, limit, skew, full):
    weights = [(1 << 20) // math.isqrt(standing ** skew) + 1 for standing in range(1, count + 1)]
    largest = limit if full else min(limit, max(-(-total // count), total * weights[0] // sum(weights)))
    least = 1 if total - largest >= count - 1 else 0
    counts, spare = [largest] + [least] * (count - 1), total - largest - least * (count - 1)
    while spare > 0:
        movable = [i for i in range(1, count) if counts[i] < largest] or [i for i in range(1, count) if counts[i] < limit]
        mass, left = sum([weights[i] for i in movable]), spare
        for i in movable:
            more = min(limit - counts[i], max(1, left * weights[i] // mass), spare)
            counts[i] = counts[i] + more
            spare = spare - more
    return np.array(counts)


def scatter_about(rng, shape, scale, most, split=(), held_as=jnp.bfloat16):
    entries = scale * jax.random.normal(rng, shape, jnp.float32)
    if split:
        entries = entries * block_scale(rng, shape, split, -0.22, 0.18)
    return jnp.clip(entries, -most, most).astype(held_as)


def setup_inputs(seed: int = 0, part: int = 0) -> dict:
    keys = jax.random.split(jax.random.key(seed), 9)
    part_keys = jax.random.split(jax.random.fold_in(keys[8], part), 9)
    tokens = scatter_about(part_keys[0], (TOKENS, D), 1.0, 6.0, ((0, 128),))
    context = scatter_about(part_keys[1], (TOKENS, D), 1.0, 6.0, ((0, 128),))
    out_proj = scatter_about(part_keys[2], (D, D), D ** -0.5, 0.125, ((0, 128),))
    norm_gain = jnp.clip(1.0 + 0.18 * jax.random.normal(part_keys[3], (D,), jnp.float32), 0.1, 1.9)
    router = scatter_about(part_keys[4], (D, EXPERTS), D ** -0.5, 0.125)
    expert_ids_keys = jax.random.split(jax.random.fold_in(part_keys[5], 1), TOKENS // TOK_DEV)
    expert_ids_turns = jax.random.permutation(jax.random.fold_in(part_keys[5], 3), TOKENS // TOK_DEV)
    expert_ids = jax.vmap(lambda own, number: assign_block(jax.random.fold_in(part_keys[5], 2), own, number, TOK_DEV, EXPERTS, 2, CAP, 2))(expert_ids_keys, expert_ids_turns).reshape((TOKENS, 2))
    w_gate_up = scatter_about(part_keys[6], (2 * EXPERTS, 2, FF // 2, D), D ** -0.5, 0.125, ((0, 128),))
    w_down = scatter_about(part_keys[7], (2 * EXPERTS, FF // 2, D), FF ** -0.5, 0.15625, ((0, 128),))
    return dict(tokens=tokens, context=context, out_proj=out_proj, norm_gain=norm_gain, router=router, expert_ids=expert_ids, w_gate_up=w_gate_up, w_down=w_down)


def reference(tokens, context, out_proj, norm_gain, router, expert_ids, w_gate_up, w_down):
    attended = jnp.dot(context, out_proj, preferred_element_type=jnp.float32)
    residual_in = (tokens.astype(jnp.float32) + attended).astype(jnp.bfloat16)
    widened = residual_in.astype(jnp.float32)
    inv_rms = lax.rsqrt(lax.optimization_barrier(jnp.mean(widened * widened, axis=1, keepdims=True)) + 1e-05)
    normed = (widened * inv_rms * norm_gain).astype(jnp.bfloat16)
    logits = jnp.dot(normed, router, preferred_element_type=jnp.float32)
    picked = jnp.take_along_axis(logits, expert_ids, axis=1)
    scores = jax.nn.sigmoid(picked)
    gate_vals = scores / lax.optimization_barrier(jnp.sum(scores, axis=1, keepdims=True))
    experts = EXPERTS
    blocks = N_EXPERT * N_FSDP
    ids_block = expert_ids.reshape(blocks, 2 * TOK_DEV)
    onehot = (ids_block[:, :, None] == jnp.arange(experts, dtype=jnp.int32)[None, None, :]).astype(jnp.int32)
    before = jnp.cumsum(onehot, axis=1) - onehot
    places = lax.optimization_barrier(jnp.sum(before * onehot, axis=2))
    block_of = jnp.arange(blocks, dtype=jnp.int32)[:, None]
    slot_index = ((ids_block * blocks + block_of) * CAP + places).reshape(-1).astype(jnp.int32)
    assign = jnp.arange(2 * TOKENS, dtype=jnp.int32)
    table_tok = jnp.full((experts * blocks * CAP,), TOKENS, jnp.int32).at[slot_index].set(assign // 2)
    table_gate = jnp.zeros((experts * blocks * CAP,), jnp.float32).at[slot_index].set(gate_vals.reshape(-1))
    padded = jnp.concatenate([normed, jnp.zeros((1, D), jnp.bfloat16)], axis=0)
    half_units = FF // 2

    def one_expert(running, inputs):
        slot_tokens, slot_gates, gate_up_w, down_w = inputs
        taken = padded[slot_tokens]
        total = jnp.zeros((taken.shape[0], D), jnp.float32)
        for half in range(2):
            gate_val = jnp.dot(taken, gate_up_w[half, 0].T, preferred_element_type=jnp.float32)
            up_val = jnp.dot(taken, gate_up_w[half, 1].T, preferred_element_type=jnp.float32)
            hidden = (jax.nn.silu(gate_val) * up_val).astype(jnp.bfloat16)
            piece = jnp.dot(hidden, down_w[half], preferred_element_type=jnp.float32).astype(jnp.bfloat16)
            piece = lax.optimization_barrier(piece)
            total = total + piece.astype(jnp.float32)
        combined = lax.optimization_barrier(total.astype(jnp.bfloat16)).astype(jnp.float32)
        running = running.at[slot_tokens].add(slot_gates[:, None] * combined)
        return (running, None)
    start_acc = jnp.zeros((TOKENS + 1, D), jnp.float32)
    running, unused = lax.scan(one_expert, start_acc, (table_tok.reshape(experts, -1), table_gate.reshape(experts, -1), w_gate_up.reshape(experts, 2, 2, half_units, D), w_down.reshape(experts, 2, half_units, D)))
    return (widened + running[:TOKENS]).astype(jnp.bfloat16)
```

```python
import functools

import jax
import jax.numpy as jnp
from jax import lax
from jax.experimental import pallas as pl
from jax.experimental.pallas import tpu as pltpu
from jax.sharding import PartitionSpec as P

eps_norm = 1e-05
MESH = pl.DeviceIdType.MESH
f32, bf16 = jnp.float32, jnp.bfloat16


def block_kernel(
    dims,
    tokens_hbm, context_hbm, shard_hbm, gain_ref, router_ref, ids_ref, gate_up_hbm, down_hbm,
    out_ref,
    proj, tok, ctx, resid, normed, gate_up, down,
    slot_rows, pick0, pick1, mask0, mask1,
    wide, outbox, inbox, rows2d, hidden, halves, others, finished,
    load_sem, pair_sem, ring1_send, ring1_recv, ring2_send, ring2_recv, copy_send, copy_recv,
    out_send, out_recv, fwd_send, fwd_recv, half_send, half_recv, home_send, home_recv,
):
    E, F, cap, chunk = dims
    T, D = out_ref.shape
    J = D // 128
    Y, pairs = E // 2, F // 2
    experts = E * pairs
    slots = experts * cap
    rem, div = lax.rem, lax.div

    c = lax.axis_index("expert")
    x = lax.axis_index("fsdp")
    y, core = div(c, 2), rem(c, 2)
    par = rem(x, 2)
    tau = 1 - 2 * par

    def dev(cc, xx):
        return {"expert": cc, "fsdp": xx}

    def wait_bytes(ref, sem):
        pltpu.make_async_copy(ref, ref, sem).wait()

    Dh = D // 2
    loads = [
        pltpu.make_async_copy(shard_hbm.at[:, h * Dh:(h + 1) * Dh], proj.at[h, y, core, x], load_sem.at[h])
        for h in range(2)
    ]
    loads.append(pltpu.make_async_copy(context_hbm, ctx, load_sem.at[2]))
    loads.append(pltpu.make_async_copy(tokens_hbm, tok, load_sem.at[3]))
    loads.append(pltpu.make_async_copy(gate_up_hbm.at[0], gate_up, load_sem.at[4]))
    loads.append(pltpu.make_async_copy(down_hbm.at[0], down, load_sem.at[5]))
    for load in loads:
        load.start()

    barrier = pltpu.get_barrier_semaphore()
    me = c * F + x

    def greet(n, carry):
        other = rem(me + n, E * F)
        pl.semaphore_signal(barrier, inc=1, device_id=dev(div(other, F), rem(other, F)), device_id_type=MESH)
        return carry

    lax.fori_loop(1, E * F, greet, 0)
    pl.semaphore_wait(barrier, E * F - 1)

    loads[0].wait()
    loads[1].wait()
    partner_core = dev(c + 1 - 2 * core, x)
    swap = pltpu.make_async_remote_copy(
        src_ref=proj.at[1 - core, y, core, x], dst_ref=proj.at[1 - core, y, core, x],
        send_sem=pair_sem.at[0], recv_sem=pair_sem.at[1], device_id=partner_core, device_id_type=MESH,
    )
    swap.start()
    own = pltpu.make_async_remote_copy(
        src_ref=proj.at[core, y, core, x], dst_ref=proj.at[core, y, core, x],
        send_sem=pair_sem.at[2], recv_sem=pair_sem.at[3], device_id=partner_core, device_id_type=MESH,
    )
    own.start()
    swap.wait_recv()

    N = F
    pos1 = x * (1 - core) + y * core
    pos2 = y * (1 - core) + x * core

    def piece(p1, p2):
        return proj.at[core, p2 * (1 - core) + p1 * core, :, p1 * (1 - core) + p2 * core]

    def at(p1, p2):
        return dev(2 * (p2 * (1 - core) + p1 * core) + core, p1 * (1 - core) + p2 * core)

    def ring1(way, step, p1):
        sign = 1 - 2 * way
        ref = piece(p1, pos2)
        return pltpu.make_async_remote_copy(
            src_ref=ref, dst_ref=ref, send_sem=ring1_send, recv_sem=ring1_recv.at[way * (N // 2) + step],
            device_id=at(rem(pos1 + sign + N, N), pos2), device_id_type=MESH,
        )

    def ring2(way, step, p1, p2, o):
        sign = 1 - 2 * way
        ref = piece(p1, p2)
        return pltpu.make_async_remote_copy(
            src_ref=ref, dst_ref=ref, send_sem=ring2_send,
            recv_sem=ring2_recv.at[(way * (N // 2) + step) * N + o],
            device_id=at(pos1, rem(pos2 + sign + N, N)), device_id_type=MESH,
        )

    def to_partner(p1, p2, which):
        ref = piece(p1, p2)
        return pltpu.make_async_remote_copy(
            src_ref=ref, dst_ref=ref, send_sem=copy_send.at[which], recv_sem=copy_recv.at[which],
            device_id=partner_core, device_id_type=MESH,
        )

    ring1(0, 0, pos1).start()
    ring1(1, 0, pos1).start()
    ring2(0, 0, pos1, pos2, 0).start()
    ring2(1, 0, pos1, pos2, 0).start()

    ids = ids_ref[...]
    expert_row = lax.broadcasted_iota(jnp.int32, (experts, T), 0)
    one0 = (expert_row == ids[0:1, :]).astype(f32)
    one1 = (expert_row == ids[1:2, :]).astype(f32)
    earlier = (
        lax.broadcasted_iota(jnp.int32, (T, T), 0) < lax.broadcasted_iota(jnp.int32, (T, T), 1)
    ).astype(bf16)
    before = jnp.dot((one0 + one1).astype(bf16), earlier, preferred_element_type=f32)
    place0 = jnp.sum(before * one0, axis=0, keepdims=True).astype(jnp.int32)
    place1 = jnp.sum(before * one1, axis=0, keepdims=True).astype(jnp.int32)
    slot_row = lax.broadcasted_iota(jnp.int32, (slots, T), 0)
    sel0 = (slot_row == ids[0:1, :] * cap + place0).astype(f32)
    sel1 = (slot_row == ids[1:2, :] * cap + place1).astype(f32)
    slot_rows[...] = (sel0 + sel1).astype(bf16)
    pick0[...] = jnp.transpose(sel0).astype(bf16)
    pick1[...] = jnp.transpose(sel1).astype(bf16)
    mask0[...] = jnp.transpose(one0)
    mask1[...] = jnp.transpose(one1)

    for step in range(1, N // 2 + 1):
        for way in range(2):
            if way == 1 and step == N // 2:
                continue
            sign = 1 - 2 * way
            p1 = rem(pos1 - sign * step + N, N)
            o = 2 * step - 1 + way
            ring1(way, step - 1, p1).wait_recv()
            if step < N // 2 - way:
                ring1(way, step, p1).start()
            ring2(0, 0, p1, pos2, o).start()
            ring2(1, 0, p1, pos2, o).start()
            to_partner(p1, pos2, 0).start()

    for step in range(1, N // 2 + 1):

        def pass_on(oo, carry, step=step):
            for odd in range(2):
                o = 2 * oo + odd
                half = div(o + 1, 2)
                p1 = rem(pos1 + (half if odd == 0 else -half) + N, N)
                for way in range(2):
                    hops = N // 2 if way == odd else N // 2 - 1
                    if step > hops:
                        continue
                    sign = 1 - 2 * way
                    p2 = rem(pos2 - sign * step + N, N)
                    ring2(way, step - 1, p1, p2, o).wait_recv()
                    if step < hops:
                        ring2(way, step, p1, p2, o).start()
                    to_partner(p1, p2, 1).start()
            return carry

        lax.fori_loop(0, N // 2, pass_on, 0)

    own.wait_recv()
    wait_bytes(proj.at[1 - core, pl.ds(0, 1), :, pl.ds(0, N - 1)], copy_recv.at[0])
    wait_bytes(proj.at[1 - core, pl.ds(0, N - 1)], copy_recv.at[1])

    loads[2].wait()
    loads[3].wait()
    wide_cols = 512 if D >= 2048 else 128
    squares = jnp.zeros((T, 1), f32)
    for n in range(D // wide_cols):
        at_col = n * wide_cols
        h, off = at_col // Dh, at_col % Dh
        weights = proj[h, :, :, :, :, off:off + wide_cols].reshape(D, wide_cols)
        attended = jnp.dot(ctx[...], weights, preferred_element_type=f32)
        cols = slice(at_col, at_col + wide_cols)
        r = (tok[:, cols].astype(f32) + attended).astype(bf16)
        resid[:, cols] = r
        r = r.astype(f32)
        squares = squares + jnp.sum(r * r, axis=1, keepdims=True)
    inv_rms = lax.rsqrt(squares * (1.0 / D) + eps_norm)
    for n in range(D // wide_cols):
        cols = slice(n * wide_cols, (n + 1) * wide_cols)
        normed[:, cols] = (resid[:, cols].astype(f32) * inv_rms * gain_ref[:, cols]).astype(bf16)

    for jj in range(J // 2):
        cols = slice(256 * jj, 256 * jj + 256)
        got = jnp.dot(slot_rows[...], normed[:, cols], preferred_element_type=f32)
        wide[0:slots, 2 * jj, :] = got[:, :128]
        wide[0:slots, 2 * jj + 1, :] = got[:, 128:]
    eb = 4

    def narrow(n, carry):
        block = wide[pl.ds(n * eb * cap, eb * cap)].astype(bf16)
        outbox[pl.ds(n * eb, eb)] = block.reshape(eb, cap, J, 128)
        return carry

    lax.fori_loop(0, experts // eb, narrow, 0)

    def shift(k):
        return div(k + 1, 2) * rem(k, 2) + rem(E - div(k, 2), E) * (1 - rem(k, 2))

    def near(i):
        return rem(x + tau * (i if i % 2 == 0 else -i) + F, F)

    def send_slot(k, i):
        to_c, to_x = rem(c + shift(k), E), near(i)
        return pltpu.make_async_remote_copy(
            src_ref=outbox.at[pairs * to_c + div(to_x, 2)], dst_ref=inbox.at[c, rem(to_x, 2), i],
            send_sem=out_send, recv_sem=out_recv.at[k], device_id=dev(to_c, to_x), device_id_type=MESH,
        )

    for i in range(pairs - 1, 0, -1):
        send_slot(0, i).start()
    inbox[c, par, 0] = outbox[pairs * c + div(x, 2)]

    def send_round(k, carry):
        for i in range(pairs - 1, -1, -1):
            send_slot(k, i).start()
        return carry

    lax.fori_loop(1, E, send_round, 0)

    logits = lax.dot_general(
        normed[...], router_ref[...], (((1,), (1,)), ((), ())), preferred_element_type=f32
    )
    score0 = 1.0 / (1.0 + jnp.exp(-jnp.sum(logits * mask0[...], axis=1, keepdims=True)))
    score1 = 1.0 / (1.0 + jnp.exp(-jnp.sum(logits * mask1[...], axis=1, keepdims=True)))
    gate0 = score0 / (score0 + score1)
    gate1 = score1 / (score0 + score1)

    partner = dev(c, x + tau)

    def source(k):
        return rem(c + E - shift(k), E)

    def forward(k):
        ref = inbox.at[source(k), par]
        return pltpu.make_async_remote_copy(
            src_ref=ref, dst_ref=ref, send_sem=fwd_send, recv_sem=fwd_recv.at[k],
            device_id=partner, device_id_type=MESH,
        )

    def pump(g):
        def one(kk, carry):
            k = g * chunk + kk
            wait_bytes(inbox.at[0, 0], out_recv.at[k])
            forward(k).start()
            return carry

        lax.fori_loop(0, chunk, one, 0)

    def pump_first():
        wait_bytes(inbox.at[0, 0, pl.ds(0, pairs - 1)], out_recv.at[0])
        forward(0).start()

        def one(k, carry):
            wait_bytes(inbox.at[0, 0], out_recv.at[k])
            forward(k).start()
            return carry

        lax.fori_loop(1, chunk, one, 0)

    per = 2 * pairs * cap
    rows = chunk * per

    def half_back(k):
        src = source(k)
        return pltpu.make_async_remote_copy(
            src_ref=halves.at[src, 1 - par], dst_ref=others.at[src], send_sem=half_send, recv_sem=half_recv.at[k],
            device_id=partner, device_id_type=MESH,
        )

    def experts_on(g):
        def take(kk, carry):
            k = g * chunk + kk
            wait_bytes(inbox.at[0, 0], fwd_recv.at[k])
            block = inbox[source(k)].reshape(per, J, 128)
            wide[pl.ds(kk * per, per)] = block.astype(f32)
            return carry

        lax.fori_loop(0, chunk, take, 0)
        for jj in range(J // 2):
            both = jnp.concatenate([wide[0:rows, 2 * jj, :], wide[0:rows, 2 * jj + 1, :]], axis=1)
            rows2d[:, 256 * jj:256 * jj + 256] = both.astype(bf16)
        over_last = (((1,), (1,)), ((), ()))
        gate = lax.dot_general(rows2d[...], gate_up[0], over_last, preferred_element_type=f32)
        up = lax.dot_general(rows2d[...], gate_up[1], over_last, preferred_element_type=f32)
        hidden[...] = (gate / (1.0 + jnp.exp(-gate)) * up).astype(bf16)
        for jj in range(J // 2):
            got = jnp.dot(hidden[...], down[:, 256 * jj:256 * jj + 256], preferred_element_type=f32)
            wide[0:rows, 2 * jj, :] = got[:, :128]
            wide[0:rows, 2 * jj + 1, :] = got[:, 128:]

        def give(kk, carry):
            k = g * chunk + kk
            block = wide[pl.ds(kk * per, per)].astype(bf16)
            halves[source(k)] = block.reshape(2, pairs, cap, J, 128)
            half_back(k).start()
            return carry

        lax.fori_loop(0, chunk, give, 0)

    mine = pairs * c + div(x, 2)

    def send_home(k, i):
        src = source(k)
        return pltpu.make_async_remote_copy(
            src_ref=halves.at[src, par, i], dst_ref=finished.at[mine], send_sem=home_send, recv_sem=home_recv,
            device_id=dev(src, rem(x - tau * i + F, F)), device_id_type=MESH,
        )

    def add_halves(k):
        src = source(k)
        wait_bytes(others.at[0], half_recv.at[k])
        total = halves[src, par].astype(f32) + others[src].astype(f32)
        halves[src, par] = total.astype(bf16)

    def finish(g):
        def one(kk, carry):
            k = g * chunk + kk
            add_halves(k)
            for i in range(pairs - 1, -1, -1):
                send_home(k, i).start()
            return carry

        lax.fori_loop(0, chunk, one, 0)

    def finish_first():
        add_halves(0)
        for i in range(pairs - 1, 0, -1):
            send_home(0, i).start()
        finished[mine] = halves[c, par, 0]

        def one(k, carry):
            add_halves(k)
            for i in range(pairs - 1, -1, -1):
                send_home(k, i).start()
            return carry

        lax.fori_loop(1, chunk, one, 0)

    loads[4].wait()
    loads[5].wait()
    groups = E // chunk
    pump_first()
    pump(1)
    experts_on(0)
    pump(2)
    experts_on(1)
    finish_first()

    def middle(g, carry):
        pump(g + 1)
        experts_on(g)
        finish(g - 1)
        return carry

    lax.fori_loop(2, groups - 1, middle, 0)
    experts_on(groups - 1)
    finish(groups - 2)
    finish(groups - 1)

    wait_bytes(finished.at[pl.ds(0, experts - 1)], home_recv)

    def widen(n, carry):
        block = finished[pl.ds(n * eb, eb)].astype(f32)
        wide[pl.ds(n * eb * cap, eb * cap)] = block.reshape(eb * cap, J, 128)
        return carry

    lax.fori_loop(0, experts // eb, widen, 0)
    for jj in range(J // 2):
        cols = slice(256 * jj, 256 * jj + 256)
        got = jnp.concatenate([wide[0:slots, 2 * jj, :], wide[0:slots, 2 * jj + 1, :]], axis=1).astype(bf16)
        first = jnp.dot(pick0[...], got, preferred_element_type=f32)
        second = jnp.dot(pick1[...], got, preferred_element_type=f32)
        out_ref[:, cols] = (resid[:, cols].astype(f32) + gate0 * first + gate1 * second).astype(bf16)

    swap.wait_send()
    own.wait_send()
    wait_bytes(proj.at[core, pl.ds(0, 1), :, pl.ds(0, N - 1)], ring1_send)
    wait_bytes(proj.at[core, pl.ds(0, N - 1)], ring2_send)
    wait_bytes(proj.at[core, pl.ds(0, 1), :, pl.ds(0, N - 1)], copy_send.at[0])
    wait_bytes(proj.at[core, pl.ds(0, N - 1)], copy_send.at[1])
    wait_bytes(outbox.at[pl.ds(0, experts - 1)], out_send)
    wait_bytes(inbox.at[:, 0], fwd_send)
    wait_bytes(others, half_send)
    wait_bytes(finished.at[pl.ds(0, experts - 1)], home_send)


def on_device(tokens, context, out_proj, norm_gain, router, expert_ids, w_gate_up, w_down):
    T, D = tokens.shape
    E, F = lax.axis_size("expert"), lax.axis_size("fsdp")
    Y, pairs = E // 2, F // 2
    experts = E * pairs
    cap = 5 * T // (2 * experts)
    J = D // 128
    R = out_proj.shape[0]
    half_units = w_down.shape[1]
    slots = experts * cap
    chunk = E // 4
    rows = chunk * 2 * pairs * cap
    N = F
    vmem, dma = pltpu.VMEM, pltpu.SemaphoreType.DMA
    any_space = pl.BlockSpec(memory_space=pl.ANY)
    in_vmem = pl.BlockSpec(memory_space=pltpu.VMEM)
    return pl.pallas_call(
        functools.partial(block_kernel, (E, F, cap, chunk)),
        out_shape=jax.ShapeDtypeStruct((T, D), bf16),
        in_specs=[any_space, any_space, any_space, in_vmem, in_vmem, in_vmem, any_space, any_space],
        out_specs=in_vmem,
        scratch_shapes=[
            vmem((2, Y, 2, F, R, D // 2), bf16),
            vmem((T, D), bf16), vmem((T, D), bf16), vmem((T, D), bf16), vmem((T, D), bf16),
            vmem((2, half_units, D), bf16), vmem((half_units, D), bf16),
            vmem((slots, T), bf16), vmem((T, slots), bf16), vmem((T, slots), bf16),
            vmem((T, experts), f32), vmem((T, experts), f32),
            vmem((max(slots, rows), J, 128), f32),
            vmem((experts, cap, J, 128), bf16),
            vmem((E, 2, pairs, cap, J, 128), bf16),
            vmem((rows, D), bf16), vmem((rows, half_units), bf16),
            vmem((E, 2, pairs, cap, J, 128), bf16),
            vmem((E, pairs, cap, J, 128), bf16),
            vmem((experts, cap, J, 128), bf16),
            dma((6,)), dma((4,)), dma, dma((N,)), dma, dma((N * N,)), dma((2,)), dma((2,)),
            dma, dma((E,)), dma, dma((E,)), dma, dma((E,)), dma, dma,
        ],
        compiler_params=pltpu.CompilerParams(
            collective_id=0, has_side_effects=True, vmem_limit_bytes=56 * 1024 * 1024
        ),
        name="block",
    )(
        tokens, context, out_proj, norm_gain.reshape(1, D), router.T, expert_ids.T, w_gate_up, w_down
    )


def solution(mesh):
    return jax.shard_map(
        on_device,
        mesh=mesh,
        in_specs=(
            P(("sweep", "expert", "fsdp"), None),
            P(("sweep", "expert", "fsdp"), None),
            P(("sweep", "expert", "fsdp"), None),
            P("sweep"),
            P("sweep", None),
            P(("sweep", "expert", "fsdp"), None),
            P(("sweep", "expert", "fsdp"), None, None, None),
            P(("sweep", "expert", "fsdp"), None, None),
        ),
        out_specs=P(("sweep", "expert", "fsdp"), None),
        check_vma=False,
    )
```

```python
import functools

import jax
import jax.numpy as jnp
from jax import lax
from jax.experimental import pallas as pl
from jax.experimental.pallas import tpu as pltpu
from jax.sharding import PartitionSpec as P

eps_norm = 1e-05
MESH = pl.DeviceIdType.MESH
f32, bf16 = jnp.float32, jnp.bfloat16


def block_kernel(
    dims,
    tokens_hbm, context_hbm, shard_hbm, gain_ref, router_ref, ids_ref, gate_up_hbm, down_hbm,
    out_ref,
    proj, tok, ctx, resid, normed, gate_up, down,
    slot_rows, picks, mask0, mask1, total,
    wide, outbox, inbox, rows2d, hidden, halves, others, finished,
    load_sem, pair_sem, ring1_send, ring1_recv, ring2_send, ring2_recv, copy_send, copy_recv,
    out_send, out_recv, fwd_send, fwd_recv, half_send, half_recv, home_send, home_recv,
):
    E, F, cap, chunk = dims
    T, D = out_ref.shape
    J = D // 128
    Y, pairs = E // 2, F // 2
    experts = E * pairs
    slots = experts * cap
    rem, div = lax.rem, lax.div

    c = lax.axis_index("expert")
    x = lax.axis_index("fsdp")
    y, core = div(c, 2), rem(c, 2)
    par = rem(x, 2)
    tau = 1 - 2 * par

    def dev(cc, xx):
        return {"expert": cc, "fsdp": xx}

    def wait_bytes(ref, sem):
        pltpu.make_async_copy(ref, ref, sem).wait()

    Dh = D // 2
    loads = [
        pltpu.make_async_copy(shard_hbm.at[:, h * Dh:(h + 1) * Dh], proj.at[h, y, core, x], load_sem.at[h])
        for h in range(2)
    ]
    loads.append(pltpu.make_async_copy(context_hbm, ctx, load_sem.at[2]))
    loads.append(pltpu.make_async_copy(tokens_hbm, tok, load_sem.at[3]))
    loads.append(pltpu.make_async_copy(gate_up_hbm.at[0], gate_up, load_sem.at[4]))
    loads.append(pltpu.make_async_copy(down_hbm.at[0], down, load_sem.at[5]))
    for load in loads:
        load.start()

    N = F
    partner_core = dev(c + 1 - 2 * core, x)
    first = [partner_core]
    first += [dev(c, rem(x + n, F)) for n in (1, F - 1)] + [dev(rem(c + n, E), x) for n in (2, E - 2)]
    barrier = pltpu.get_barrier_semaphore()
    for other in first:
        pl.semaphore_signal(barrier, inc=1, device_id=other, device_id_type=MESH)
    pl.semaphore_wait(barrier, len(first))

    loads[0].wait()
    loads[1].wait()
    swap = pltpu.make_async_remote_copy(
        src_ref=proj.at[1 - core, y, core, x], dst_ref=proj.at[1 - core, y, core, x],
        send_sem=pair_sem.at[0], recv_sem=pair_sem.at[1], device_id=partner_core, device_id_type=MESH,
    )
    swap.start()
    own = pltpu.make_async_remote_copy(
        src_ref=proj.at[core, y, core, x], dst_ref=proj.at[core, y, core, x],
        send_sem=pair_sem.at[2], recv_sem=pair_sem.at[3], device_id=partner_core, device_id_type=MESH,
    )
    own.start()
    swap.wait_recv()

    pos1 = x * (1 - core) + y * core
    pos2 = y * (1 - core) + x * core

    def piece(p1, p2):
        return proj.at[core, p2 * (1 - core) + p1 * core, :, p1 * (1 - core) + p2 * core]

    def at(p1, p2):
        return dev(2 * (p2 * (1 - core) + p1 * core) + core, p1 * (1 - core) + p2 * core)

    def ring1(way, step, p1):
        sign = 1 - 2 * way
        ref = piece(p1, pos2)
        return pltpu.make_async_remote_copy(
            src_ref=ref, dst_ref=ref, send_sem=ring1_send, recv_sem=ring1_recv.at[way * (N // 2) + step],
            device_id=at(rem(pos1 + sign + N, N), pos2), device_id_type=MESH,
        )

    def ring2(way, step, p1, p2, o):
        sign = 1 - 2 * way
        ref = piece(p1, p2)
        return pltpu.make_async_remote_copy(
            src_ref=ref, dst_ref=ref, send_sem=ring2_send,
            recv_sem=ring2_recv.at[(way * (N // 2) + step) * N + o],
            device_id=at(pos1, rem(pos2 + sign + N, N)), device_id_type=MESH,
        )

    def to_partner(p1, p2, which):
        ref = piece(p1, p2)
        return pltpu.make_async_remote_copy(
            src_ref=ref, dst_ref=ref, send_sem=copy_send.at[which], recv_sem=copy_recv.at[which],
            device_id=partner_core, device_id_type=MESH,
        )

    ring2(0, 0, pos1, pos2, 0).start()
    ring2(1, 0, pos1, pos2, 0).start()
    for way in range(2):
        ring1(way, 0, pos1).start()

    ids = ids_ref[...]
    expert_row = lax.broadcasted_iota(jnp.int32, (experts, T), 0)
    one0 = (expert_row == ids[0:1, :]).astype(f32)
    one1 = (expert_row == ids[1:2, :]).astype(f32)
    earlier = (
        lax.broadcasted_iota(jnp.int32, (T, T), 0) < lax.broadcasted_iota(jnp.int32, (T, T), 1)
    ).astype(bf16)
    before = jnp.dot((one0 + one1).astype(bf16), earlier, preferred_element_type=f32)
    place0 = jnp.sum(before * one0, axis=0, keepdims=True).astype(jnp.int32)
    place1 = jnp.sum(before * one1, axis=0, keepdims=True).astype(jnp.int32)
    slot_row = lax.broadcasted_iota(jnp.int32, (slots, T), 0)
    sel0 = (slot_row == ids[0:1, :] * cap + place0).astype(f32)
    sel1 = (slot_row == ids[1:2, :] * cap + place1).astype(f32)
    slot_rows[...] = (sel0 + sel1).astype(bf16)
    expert = lax.broadcasted_iota(jnp.int32, (experts, 1), 0)
    ahead = jnp.right_shift(expert, pairs.bit_length() - 1) - c
    ahead = jnp.where(ahead < 0, ahead + E, ahead)
    turn_of = jnp.where(ahead > E // 2, 2 * (E - ahead), 2 * ahead - jnp.minimum(ahead, 1))
    start = (turn_of * (pairs * cap) + jnp.bitwise_and(expert, pairs - 1) * cap).astype(f32)
    home0 = jnp.sum((before + start) * one0, axis=0, keepdims=True).astype(jnp.int32)
    home1 = jnp.sum((before + start) * one1, axis=0, keepdims=True).astype(jnp.int32)
    part = chunk * pairs * cap
    for n, home in enumerate((home0, home1)):
        chosen = jnp.transpose((slot_row == home).astype(f32)).astype(bf16)
        for g in range(E // chunk):
            picks[g, n * T:(n + 1) * T, :] = chosen[:, g * part:(g + 1) * part]
    mask0[...] = jnp.transpose(one0)
    mask1[...] = jnp.transpose(one1)

    def pass_on(o, step):
        p1 = rem(pos1 + (o // 2 if o % 2 == 0 else N - (o + 1) // 2), N)
        for way in range(2):
            hops = N // 2 if way == o % 2 else N // 2 - 1
            if step > hops:
                continue
            p2 = rem(pos2 + (N - step if way == 0 else step), N)
            ring2(way, step - 1, p1, p2, o).wait_recv()
            if step < hops:
                ring2(way, step, p1, p2, o).start()
            to_partner(p1, p2, 1).start()

    for slot in range(1, N + 1):
        if slot <= N // 2:
            for way in range(2):
                if way == 1 and slot == N // 2:
                    continue
                p1 = rem(pos1 + (N - slot if way == 0 else slot), N)
                o = 2 * slot - 1 + way
                ring1(way, slot - 1, p1).wait_recv()
                if slot < N // 2 - way:
                    ring1(way, slot, p1).start()
                ring2(0, 0, p1, pos2, o).start()
                ring2(1, 0, p1, pos2, o).start()
                to_partner(p1, pos2, 0).start()
        for o in range(N):
            step = slot - (o + 1) // 2
            if 1 <= step <= N // 2:
                pass_on(o, step)

    loads[2].wait()
    loads[3].wait()
    wide_cols = 512 if D >= 2048 else 128
    squares = jnp.zeros((T, 1), f32)
    for turn in range(2):
        h = core if turn == 0 else 1 - core
        if turn == 1:
            own.wait_recv()
            wait_bytes(proj.at[1 - core, pl.ds(0, 1), :, pl.ds(0, N - 1)], copy_recv.at[0])
            wait_bytes(proj.at[1 - core, pl.ds(0, N - 1)], copy_recv.at[1])
        for off in range(0, Dh, wide_cols):
            weights = proj[h, :, :, :, :, off:off + wide_cols].reshape(D, wide_cols)
            attended = jnp.dot(ctx[...], weights, preferred_element_type=f32)
            cols = pl.ds(pl.multiple_of(h * Dh + off, wide_cols), wide_cols)
            r = (tok[:, cols].astype(f32) + attended).astype(bf16)
            resid[:, cols] = r
            r = r.astype(f32)
            squares = squares + jnp.sum(r * r, axis=1, keepdims=True)
    inv_rms = lax.rsqrt(squares * (1.0 / D) + eps_norm)
    for n in range(D // wide_cols):
        cols = slice(n * wide_cols, (n + 1) * wide_cols)
        normed[:, cols] = (resid[:, cols].astype(f32) * inv_rms * gain_ref[:, cols]).astype(bf16)

    for jj in range(J // 2):
        cols = slice(256 * jj, 256 * jj + 256)
        got = jnp.dot(slot_rows[...], normed[:, cols], preferred_element_type=f32)
        wide[0:slots, 2 * jj, :] = got[:, :128]
        wide[0:slots, 2 * jj + 1, :] = got[:, 128:]
    eb = 4

    def narrow(n, carry):
        block = wide[pl.ds(n * eb * cap, eb * cap)].astype(bf16)
        outbox[pl.ds(n * eb, eb)] = block.reshape(eb, cap, J, 128)
        return carry

    lax.fori_loop(0, experts // eb, narrow, 0)

    def shift(k):
        return div(k + 1, 2) * rem(k, 2) + rem(E - div(k, 2), E) * (1 - rem(k, 2))

    def near(i):
        return rem(x + tau * (i if i % 2 == 0 else -i) + F, F)

    def send_slot(k, i):
        to_c, to_x = rem(c + shift(k), E), near(i)
        return pltpu.make_async_remote_copy(
            src_ref=outbox.at[pairs * to_c + div(to_x, 2)], dst_ref=inbox.at[c, rem(to_x, 2), i],
            send_sem=out_send, recv_sem=out_recv.at[k], device_id=dev(to_c, to_x), device_id_type=MESH,
        )

    for i in range(pairs - 1, 0, -1):
        send_slot(0, i).start()
    inbox[c, par, 0] = outbox[pairs * c + div(x, 2)]

    def send_round(k, carry):
        for i in range(pairs - 1, -1, -1):
            send_slot(k, i).start()
        return carry

    lax.fori_loop(1, E, send_round, 0)

    logits = lax.dot_general(
        normed[...], router_ref[...], (((1,), (1,)), ((), ())), preferred_element_type=f32
    )
    score0 = 1.0 / (1.0 + jnp.exp(-jnp.sum(logits * mask0[...], axis=1, keepdims=True)))
    score1 = 1.0 / (1.0 + jnp.exp(-jnp.sum(logits * mask1[...], axis=1, keepdims=True)))
    gate0 = score0 / (score0 + score1)
    gate1 = score1 / (score0 + score1)

    partner = dev(c, x + tau)

    def source(k):
        return rem(c + E - shift(k), E)

    def forward(k):
        ref = inbox.at[source(k), par]
        return pltpu.make_async_remote_copy(
            src_ref=ref, dst_ref=ref, send_sem=fwd_send, recv_sem=fwd_recv.at[k],
            device_id=partner, device_id_type=MESH,
        )

    def pump(g):
        def one(kk, carry):
            k = g * chunk + kk
            wait_bytes(inbox.at[0, 0], out_recv.at[k])
            forward(k).start()
            return carry

        lax.fori_loop(0, chunk, one, 0)

    def pump_first():
        wait_bytes(inbox.at[0, 0, pl.ds(0, pairs - 1)], out_recv.at[0])
        forward(0).start()

        def one(k, carry):
            wait_bytes(inbox.at[0, 0], out_recv.at[k])
            forward(k).start()
            return carry

        lax.fori_loop(1, chunk, one, 0)

    per = 2 * pairs * cap
    rows = chunk * per

    def half_back(k):
        src = source(k)
        return pltpu.make_async_remote_copy(
            src_ref=halves.at[src, 1 - par], dst_ref=others.at[src], send_sem=half_send, recv_sem=half_recv.at[k],
            device_id=partner, device_id_type=MESH,
        )

    def experts_on(g):
        def take(kk, carry):
            k = g * chunk + kk
            wait_bytes(inbox.at[0, 0], fwd_recv.at[k])
            block = inbox[source(k)].reshape(per, J, 128)
            wide[pl.ds(kk * per, per)] = block.astype(f32)
            return carry

        lax.fori_loop(0, chunk, take, 0)
        for jj in range(J // 2):
            both = jnp.concatenate([wide[0:rows, 2 * jj, :], wide[0:rows, 2 * jj + 1, :]], axis=1)
            rows2d[:, 256 * jj:256 * jj + 256] = both.astype(bf16)
        over_last = (((1,), (1,)), ((), ()))
        gate = lax.dot_general(rows2d[...], gate_up[0], over_last, preferred_element_type=f32)
        up = lax.dot_general(rows2d[...], gate_up[1], over_last, preferred_element_type=f32)
        hidden[...] = (gate / (1.0 + jnp.exp(-gate)) * up).astype(bf16)
        for jj in range(J // 2):
            got = jnp.dot(hidden[...], down[:, 256 * jj:256 * jj + 256], preferred_element_type=f32)
            wide[0:rows, 2 * jj, :] = got[:, :128]
            wide[0:rows, 2 * jj + 1, :] = got[:, 128:]

        def give(kk, carry):
            k = g * chunk + kk
            block = wide[pl.ds(kk * per, per)].astype(bf16)
            halves[source(k)] = block.reshape(2, pairs, cap, J, 128)
            if g > 0:
                half_back(k).start()
            return carry

        lax.fori_loop(0, chunk, give, 0)

    mine = div(x, 2)

    def send_home(k, i):
        src = source(k)
        return pltpu.make_async_remote_copy(
            src_ref=halves.at[src, par, i], dst_ref=finished.at[k, mine], send_sem=home_send,
            recv_sem=home_recv.at[k],
            device_id=dev(src, rem(x - tau * i + F, F)), device_id_type=MESH,
        )

    def add_halves(k):
        src = source(k)
        wait_bytes(others.at[0], half_recv.at[k])
        both = halves[src, par].astype(f32) + others[src].astype(f32)
        halves[src, par] = both.astype(bf16)

    def finish(g):
        def one(kk, carry):
            k = g * chunk + kk
            add_halves(k)
            for i in range(pairs - 1, -1, -1):
                send_home(k, i).start()
            return carry

        lax.fori_loop(0, chunk, one, 0)

    def finish_first():
        add_halves(0)
        for i in range(pairs - 1, 0, -1):
            send_home(0, i).start()
        finished[0, mine] = halves[c, par, 0]

        def one(k, carry):
            add_halves(k)
            for i in range(pairs - 1, -1, -1):
                send_home(k, i).start()
            return carry

        lax.fori_loop(1, chunk, one, 0)

    loads[4].wait()
    loads[5].wait()
    groups = E // chunk

    def go_back(k, carry):
        half_back(k).start()
        return carry

    pump_first()
    pump(1)
    for g in range(groups):
        if g + 2 < groups:
            pump(g + 2)
        experts_on(g)
        if g == groups - 1:
            lax.fori_loop(0, chunk, go_back, 0)
        if g > 1:
            finish(g - 1)

    finish(groups - 1)
    finish_first()

    def widen(k):
        wide[pl.ds(rem(k, chunk) * pairs * cap, pairs * cap)] = finished[k].reshape(pairs * cap, J, 128).astype(f32)

    def arrived(k, carry):
        wait_bytes(finished.at[0], home_recv.at[k])
        widen(k)
        return carry

    for g in list(range(1, groups)) + [0]:
        if g == 0:
            wait_bytes(finished.at[0, pl.ds(0, pairs - 1)], home_recv.at[0])
            widen(0)
        lax.fori_loop(max(1, g * chunk), (g + 1) * chunk, arrived, 0)
        for jj in range(J // 2):
            cols = slice(256 * jj, 256 * jj + 256)
            got = jnp.concatenate([wide[0:part, 2 * jj, :], wide[0:part, 2 * jj + 1, :]], axis=1).astype(bf16)
            picked = jnp.dot(picks[g], got, preferred_element_type=f32)
            so_far = resid[:, cols].astype(f32) if g == 1 else total[:, cols]
            so_far = so_far + gate0 * picked[:T] + gate1 * picked[T:]
            if g > 0:
                total[:, cols] = so_far
            else:
                out_ref[:, cols] = so_far.astype(bf16)

    swap.wait_send()
    own.wait_send()
    wait_bytes(proj.at[core, pl.ds(0, 1), :, pl.ds(0, N - 1)], ring1_send)
    wait_bytes(proj.at[core, pl.ds(0, N - 1)], ring2_send)
    wait_bytes(proj.at[core, pl.ds(0, 1), :, pl.ds(0, N - 1)], copy_send.at[0])
    wait_bytes(proj.at[core, pl.ds(0, N - 1)], copy_send.at[1])
    wait_bytes(outbox.at[pl.ds(0, experts - 1)], out_send)
    wait_bytes(inbox.at[:, 0], fwd_send)
    wait_bytes(others, half_send)
    wait_bytes(outbox.at[pl.ds(0, experts - 1)], home_send)


def on_device(tokens, context, out_proj, norm_gain, router, expert_ids, w_gate_up, w_down):
    T, D = tokens.shape
    E, F = lax.axis_size("expert"), lax.axis_size("fsdp")
    Y, pairs = E // 2, F // 2
    experts = E * pairs
    cap = 5 * T // (2 * experts)
    J = D // 128
    R = out_proj.shape[0]
    half_units = w_down.shape[1]
    slots = experts * cap
    chunk = E // 4
    rows = chunk * 2 * pairs * cap
    N = F
    vmem, dma = pltpu.VMEM, pltpu.SemaphoreType.DMA
    any_space = pl.BlockSpec(memory_space=pl.ANY)
    in_vmem = pl.BlockSpec(memory_space=pltpu.VMEM)
    return pl.pallas_call(
        functools.partial(block_kernel, (E, F, cap, chunk)),
        out_shape=pltpu.VMEM((T, D), bf16),
        in_specs=[any_space, any_space, any_space, in_vmem, in_vmem, in_vmem, any_space, any_space],
        out_specs=in_vmem,
        scratch_shapes=[
            vmem((2, Y, 2, F, R, D // 2), bf16),
            vmem((T, D), bf16), vmem((T, D), bf16), vmem((T, D), bf16), vmem((T, D), bf16),
            vmem((2, half_units, D), bf16), vmem((half_units, D), bf16),
            vmem((slots, T), bf16), vmem((E // chunk, 2 * T, chunk * pairs * cap), bf16),
            vmem((T, experts), f32), vmem((T, experts), f32), vmem((T, D), f32),
            vmem((max(slots, rows), J, 128), f32),
            vmem((experts, cap, J, 128), bf16),
            vmem((E, 2, pairs, cap, J, 128), bf16),
            vmem((rows, D), bf16), vmem((rows, half_units), bf16),
            vmem((E, 2, pairs, cap, J, 128), bf16),
            vmem((E, pairs, cap, J, 128), bf16),
            vmem((E, pairs, cap, J, 128), bf16),
            dma((6,)), dma((4,)), dma, dma((N,)), dma, dma((N * N,)), dma((2,)), dma((2,)),
            dma, dma((E,)), dma, dma((E,)), dma, dma((E,)), dma, dma((E,)),
        ],
        compiler_params=pltpu.CompilerParams(
            collective_id=0, has_side_effects=True, vmem_limit_bytes=56 * 1024 * 1024
        ),
        name="block",
    )(
        tokens, context, out_proj, norm_gain.reshape(1, D), router.T, expert_ids.T, w_gate_up, w_down
    )


def solution(mesh):
    return jax.shard_map(
        on_device,
        mesh=mesh,
        in_specs=(
            P(("sweep", "expert", "fsdp"), None),
            P(("sweep", "expert", "fsdp"), None),
            P(("sweep", "expert", "fsdp"), None),
            P("sweep"),
            P("sweep", None),
            P(("sweep", "expert", "fsdp"), None),
            P(("sweep", "expert", "fsdp"), None, None, None),
            P(("sweep", "expert", "fsdp"), None, None),
        ),
        out_specs=P(("sweep", "expert", "fsdp"), None),
        check_vma=False,
    )
```

```python
import functools

import jax
import jax.numpy as jnp
from jax import lax
from jax.experimental import pallas as pl
from jax.experimental.pallas import tpu as pltpu
from jax.sharding import PartitionSpec as P

eps_norm = 1e-05
MESH = pl.DeviceIdType.MESH
f32, bf16 = jnp.float32, jnp.bfloat16


def block_kernel(
    dims,
    tokens_hbm, context_hbm, shard_hbm, gain_ref, router_ref, ids_ref, gate_up_hbm, down_hbm,
    out_ref,
    proj, tok, ctx, resid, normed, gate_up, down,
    slot_rows, picks, mask0, mask1, total,
    wide, outbox, inbox, rows2d, hidden, halves, others, finished,
    load_sem, pair_sem, ring1_send, ring1_recv, ring2_send, ring2_recv, copy_send, copy_recv,
    out_send, out_recv, fwd_send, fwd_recv, half_send, half_recv, home_send, home_recv,
):
    E, F, cap, chunk = dims
    T, D = out_ref.shape
    J = D // 128
    Y, pairs = E // 2, F // 2
    experts = E * pairs
    slots = experts * cap
    rem, div = lax.rem, lax.div

    c = lax.axis_index("expert")
    x = lax.axis_index("fsdp")
    y, core = div(c, 2), rem(c, 2)
    par = rem(x, 2)
    tau = 1 - 2 * par

    def dev(cc, xx):
        return {"expert": cc, "fsdp": xx}

    def wait_bytes(ref, sem):
        pltpu.make_async_copy(ref, ref, sem).wait()

    Dh = D // 2
    loads = [
        pltpu.make_async_copy(shard_hbm.at[:, h * Dh:(h + 1) * Dh], proj.at[h, y, core, x], load_sem.at[h])
        for h in range(2)
    ]
    loads.append(pltpu.make_async_copy(context_hbm, ctx, load_sem.at[2]))
    loads.append(pltpu.make_async_copy(tokens_hbm, tok, load_sem.at[3]))
    loads.append(pltpu.make_async_copy(gate_up_hbm.at[0], gate_up, load_sem.at[4]))
    loads.append(pltpu.make_async_copy(down_hbm.at[0], down, load_sem.at[5]))
    for load in loads:
        load.start()

    N = F
    partner_core = dev(c + 1 - 2 * core, x)
    first = [partner_core]
    first += [dev(c, rem(x + n, F)) for n in (1, F - 1)] + [dev(rem(c + n, E), x) for n in (2, E - 2)]
    barrier = pltpu.get_barrier_semaphore()
    for other in first:
        pl.semaphore_signal(barrier, inc=1, device_id=other, device_id_type=MESH)
    pl.semaphore_wait(barrier, len(first))

    loads[0].wait()
    loads[1].wait()
    swap = pltpu.make_async_remote_copy(
        src_ref=proj.at[1 - core, y, core, x], dst_ref=proj.at[1 - core, y, core, x],
        send_sem=pair_sem.at[0], recv_sem=pair_sem.at[1], device_id=partner_core, device_id_type=MESH,
    )
    swap.start()
    own = pltpu.make_async_remote_copy(
        src_ref=proj.at[core, y, core, x], dst_ref=proj.at[core, y, core, x],
        send_sem=pair_sem.at[2], recv_sem=pair_sem.at[3], device_id=partner_core, device_id_type=MESH,
    )
    own.start()
    swap.wait_recv()

    pos1 = x * (1 - core) + y * core
    pos2 = y * (1 - core) + x * core

    def piece(p1, p2):
        return proj.at[core, p2 * (1 - core) + p1 * core, :, p1 * (1 - core) + p2 * core]

    def at(p1, p2):
        return dev(2 * (p2 * (1 - core) + p1 * core) + core, p1 * (1 - core) + p2 * core)

    def ring1(way, step, p1):
        sign = 1 - 2 * way
        ref = piece(p1, pos2)
        return pltpu.make_async_remote_copy(
            src_ref=ref, dst_ref=ref, send_sem=ring1_send, recv_sem=ring1_recv.at[way * (N // 2) + step],
            device_id=at(rem(pos1 + sign + N, N), pos2), device_id_type=MESH,
        )

    def ring2(way, step, p1, p2, o):
        sign = 1 - 2 * way
        ref = piece(p1, p2)
        return pltpu.make_async_remote_copy(
            src_ref=ref, dst_ref=ref, send_sem=ring2_send,
            recv_sem=ring2_recv.at[(way * (N // 2) + step) * N + o],
            device_id=at(pos1, rem(pos2 + sign + N, N)), device_id_type=MESH,
        )

    def to_partner(p1, p2, which):
        ref = piece(p1, p2)
        return pltpu.make_async_remote_copy(
            src_ref=ref, dst_ref=ref, send_sem=copy_send.at[which], recv_sem=copy_recv.at[which],
            device_id=partner_core, device_id_type=MESH,
        )

    ring2(0, 0, pos1, pos2, 0).start()
    ring2(1, 0, pos1, pos2, 0).start()
    for way in range(2):
        ring1(way, 0, pos1).start()

    ids = ids_ref[...]
    expert_row = lax.broadcasted_iota(jnp.int32, (experts, T), 0)
    one0 = (expert_row == ids[0:1, :]).astype(f32)
    one1 = (expert_row == ids[1:2, :]).astype(f32)
    earlier = (
        lax.broadcasted_iota(jnp.int32, (T, T), 0) < lax.broadcasted_iota(jnp.int32, (T, T), 1)
    ).astype(bf16)
    before = jnp.dot((one0 + one1).astype(bf16), earlier, preferred_element_type=f32)
    place0 = jnp.sum(before * one0, axis=0, keepdims=True).astype(jnp.int32)
    place1 = jnp.sum(before * one1, axis=0, keepdims=True).astype(jnp.int32)
    slot_row = lax.broadcasted_iota(jnp.int32, (slots, T), 0)
    sel0 = (slot_row == ids[0:1, :] * cap + place0).astype(f32)
    sel1 = (slot_row == ids[1:2, :] * cap + place1).astype(f32)
    slot_rows[...] = (sel0 + sel1).astype(bf16)
    expert = lax.broadcasted_iota(jnp.int32, (experts, 1), 0)
    ahead = jnp.right_shift(expert, pairs.bit_length() - 1) - c
    ahead = jnp.where(ahead < 0, ahead + E, ahead)
    turn_of = jnp.where(ahead > E // 2, 2 * (E - ahead), 2 * ahead - jnp.minimum(ahead, 1))
    start = (turn_of * (pairs * cap) + jnp.bitwise_and(expert, pairs - 1) * cap).astype(f32)
    home0 = jnp.sum((before + start) * one0, axis=0, keepdims=True).astype(jnp.int32)
    home1 = jnp.sum((before + start) * one1, axis=0, keepdims=True).astype(jnp.int32)
    part = chunk * pairs * cap
    for n, home in enumerate((home0, home1)):
        chosen = jnp.transpose((slot_row == home).astype(f32)).astype(bf16)
        for g in range(E // chunk):
            picks[g, n * T:(n + 1) * T, :] = chosen[:, g * part:(g + 1) * part]
    mask0[...] = jnp.transpose(one0)
    mask1[...] = jnp.transpose(one1)

    def pass_on(o, step, last):
        p1 = rem(pos1 + (o // 2 if o % 2 == 0 else N - (o + 1) // 2), N)
        for way in range(2):
            hops = N // 2 if way == o % 2 else N // 2 - 1
            if step > hops or last != (step == hops):
                continue
            p2 = rem(pos2 + (N - step if way == 0 else step), N)
            ring2(way, step - 1, p1, p2, o).wait_recv()
            if step < hops:
                ring2(way, step, p1, p2, o).start()
            to_partner(p1, p2, 1).start()

    for slot in range(1, N + 1 + 1):
        if slot <= N // 2:
            for way in range(2):
                if way == 1 and slot == N // 2:
                    continue
                p1 = rem(pos1 + (N - slot if way == 0 else slot), N)
                o = 2 * slot - 1 + way
                ring1(way, slot - 1, p1).wait_recv()
                if slot < N // 2 - way:
                    ring1(way, slot, p1).start()
                ring2(0, 0, p1, pos2, o).start()
                ring2(1, 0, p1, pos2, o).start()
                to_partner(p1, pos2, 0).start()
        for o in range(N - 1, -1, -1):
            step = slot - (o + 1) // 2
            if 1 <= step < N // 2:
                pass_on(o, step, False)
        for o in range(N):
            step = slot - 1 - (o + 1) // 2
            if N // 2 - 1 <= step <= N // 2:
                pass_on(o, step, True)

    loads[2].wait()
    loads[3].wait()
    wide_cols = 512 if D >= 2048 else 128
    squares = jnp.zeros((T, 1), f32)
    for turn in range(2):
        h = core if turn == 0 else 1 - core
        if turn == 1:
            own.wait_recv()
            wait_bytes(proj.at[1 - core, pl.ds(0, 1), :, pl.ds(0, N - 1)], copy_recv.at[0])
            wait_bytes(proj.at[1 - core, pl.ds(0, N - 1)], copy_recv.at[1])
        for off in range(0, Dh, wide_cols):
            weights = proj[h, :, :, :, :, off:off + wide_cols].reshape(D, wide_cols)
            attended = jnp.dot(ctx[...], weights, preferred_element_type=f32)
            cols = pl.ds(pl.multiple_of(h * Dh + off, wide_cols), wide_cols)
            r = (tok[:, cols].astype(f32) + attended).astype(bf16)
            resid[:, cols] = r
            r = r.astype(f32)
            squares = squares + jnp.sum(r * r, axis=1, keepdims=True)
    inv_rms = lax.rsqrt(squares * (1.0 / D) + eps_norm)
    for n in range(D // wide_cols):
        cols = slice(n * wide_cols, (n + 1) * wide_cols)
        normed[:, cols] = (resid[:, cols].astype(f32) * inv_rms * gain_ref[:, cols]).astype(bf16)

    for jj in range(J // 2):
        cols = slice(256 * jj, 256 * jj + 256)
        got = jnp.dot(slot_rows[...], normed[:, cols], preferred_element_type=f32)
        wide[0:slots, 2 * jj, :] = got[:, :128]
        wide[0:slots, 2 * jj + 1, :] = got[:, 128:]
    eb = 4

    def narrow(n, carry):
        block = wide[pl.ds(n * eb * cap, eb * cap)].astype(bf16)
        outbox[pl.ds(n * eb, eb)] = block.reshape(eb, cap, J, 128)
        return carry

    lax.fori_loop(0, experts // eb, narrow, 0)

    def shift(k):
        return div(k + 1, 2) * rem(k, 2) + rem(E - div(k, 2), E) * (1 - rem(k, 2))

    def near(i):
        return rem(x + tau * (i if i % 2 == 0 else -i) + F, F)

    def send_slot(k, i):
        to_c, to_x = rem(c + shift(k), E), near(i)
        return pltpu.make_async_remote_copy(
            src_ref=outbox.at[pairs * to_c + div(to_x, 2)], dst_ref=inbox.at[c, rem(to_x, 2), i],
            send_sem=out_send, recv_sem=out_recv.at[k], device_id=dev(to_c, to_x), device_id_type=MESH,
        )

    for i in range(pairs - 1, 0, -1):
        send_slot(0, i).start()
    inbox[c, par, 0] = outbox[pairs * c + div(x, 2)]

    def send_round(k, carry):
        for i in range(pairs - 1, -1, -1):
            send_slot(k, i).start()
        return carry

    lax.fori_loop(1, E, send_round, 0)

    logits = lax.dot_general(
        normed[...], router_ref[...], (((1,), (1,)), ((), ())), preferred_element_type=f32
    )
    score0 = 1.0 / (1.0 + jnp.exp(-jnp.sum(logits * mask0[...], axis=1, keepdims=True)))
    score1 = 1.0 / (1.0 + jnp.exp(-jnp.sum(logits * mask1[...], axis=1, keepdims=True)))
    gate0 = score0 / (score0 + score1)
    gate1 = score1 / (score0 + score1)

    partner = dev(c, x + tau)

    def source(k):
        return rem(c + E - shift(k), E)

    def forward(k):
        ref = inbox.at[source(k), par]
        return pltpu.make_async_remote_copy(
            src_ref=ref, dst_ref=ref, send_sem=fwd_send, recv_sem=fwd_recv.at[k],
            device_id=partner, device_id_type=MESH,
        )

    def pump(g):
        def one(kk, carry):
            k = g * chunk + kk
            wait_bytes(inbox.at[0, 0], out_recv.at[k])
            forward(k).start()
            return carry

        lax.fori_loop(0, chunk, one, 0)

    def pump_first():
        wait_bytes(inbox.at[0, 0, pl.ds(0, pairs - 1)], out_recv.at[0])
        forward(0).start()

        def one(k, carry):
            wait_bytes(inbox.at[0, 0], out_recv.at[k])
            forward(k).start()
            return carry

        lax.fori_loop(1, chunk, one, 0)

    per = 2 * pairs * cap
    rows = chunk * per

    def half_back(k):
        src = source(k)
        return pltpu.make_async_remote_copy(
            src_ref=halves.at[src, 1 - par], dst_ref=others.at[src], send_sem=half_send, recv_sem=half_recv.at[k],
            device_id=partner, device_id_type=MESH,
        )

    def experts_on(g):
        def take(kk, carry):
            k = g * chunk + kk
            wait_bytes(inbox.at[0, 0], fwd_recv.at[k])
            block = inbox[source(k)].reshape(per, J, 128)
            wide[pl.ds(kk * per, per)] = block.astype(f32)
            return carry

        lax.fori_loop(0, chunk, take, 0)
        for jj in range(J // 2):
            both = jnp.concatenate([wide[0:rows, 2 * jj, :], wide[0:rows, 2 * jj + 1, :]], axis=1)
            rows2d[:, 256 * jj:256 * jj + 256] = both.astype(bf16)
        over_last = (((1,), (1,)), ((), ()))
        gate = lax.dot_general(rows2d[...], gate_up[0], over_last, preferred_element_type=f32)
        up = lax.dot_general(rows2d[...], gate_up[1], over_last, preferred_element_type=f32)
        hidden[...] = (gate / (1.0 + jnp.exp(-gate)) * up).astype(bf16)
        for jj in range(J // 2):
            got = jnp.dot(hidden[...], down[:, 256 * jj:256 * jj + 256], preferred_element_type=f32)
            wide[0:rows, 2 * jj, :] = got[:, :128]
            wide[0:rows, 2 * jj + 1, :] = got[:, 128:]

        def give(kk, carry):
            k = g * chunk + kk
            block = wide[pl.ds(kk * per, per)].astype(bf16)
            halves[source(k)] = block.reshape(2, pairs, cap, J, 128)
            if g > 0:
                half_back(k).start()
            return carry

        lax.fori_loop(0, chunk, give, 0)

    mine = div(x, 2)

    def send_home(k, i):
        src = source(k)
        return pltpu.make_async_remote_copy(
            src_ref=halves.at[src, par, i], dst_ref=finished.at[k, mine], send_sem=home_send,
            recv_sem=home_recv.at[k],
            device_id=dev(src, rem(x - tau * i + F, F)), device_id_type=MESH,
        )

    def add_halves(k):
        src = source(k)
        wait_bytes(others.at[0], half_recv.at[k])
        both = halves[src, par].astype(f32) + others[src].astype(f32)
        halves[src, par] = both.astype(bf16)

    def finish(g):
        def one(kk, carry):
            k = g * chunk + kk
            add_halves(k)
            for i in range(pairs - 1, -1, -1):
                send_home(k, i).start()
            return carry

        lax.fori_loop(0, chunk, one, 0)

    def finish_first():
        add_halves(0)
        for i in range(pairs - 1, 0, -1):
            send_home(0, i).start()
        finished[0, mine] = halves[c, par, 0]

        def one(k, carry):
            add_halves(k)
            for i in range(pairs - 1, -1, -1):
                send_home(k, i).start()
            return carry

        lax.fori_loop(1, chunk, one, 0)

    loads[4].wait()
    loads[5].wait()
    groups = E // chunk

    def widen(k):
        wide[pl.ds(rem(k, chunk) * pairs * cap, pairs * cap)] = finished[k].reshape(pairs * cap, J, 128).astype(f32)

    def arrived(k, carry):
        wait_bytes(finished.at[0], home_recv.at[k])
        widen(k)
        return carry

    def combine(g):
        if g == 0:
            wait_bytes(finished.at[0, pl.ds(0, pairs - 1)], home_recv.at[0])
            widen(0)
        lax.fori_loop(max(1, g * chunk), (g + 1) * chunk, arrived, 0)
        for jj in range(J // 2):
            cols = slice(256 * jj, 256 * jj + 256)
            got = jnp.concatenate([wide[0:part, 2 * jj, :], wide[0:part, 2 * jj + 1, :]], axis=1).astype(bf16)
            picked = jnp.dot(picks[g], got, preferred_element_type=f32)
            so_far = resid[:, cols].astype(f32) if g == 1 else total[:, cols]
            so_far = so_far + gate0 * picked[:T] + gate1 * picked[T:]
            if g > 0:
                total[:, cols] = so_far
            else:
                out_ref[:, cols] = so_far.astype(bf16)


    def go_back(k, carry):
        half_back(k).start()
        return carry

    pump_first()
    pump(1)
    for g in range(groups):
        if g + 2 < groups:
            pump(g + 2)
        experts_on(g)
        if g == groups - 1:
            lax.fori_loop(0, chunk, go_back, 0)
        if g > 1:
            finish(g - 1)

    finish(groups - 1)
    for g in range(1, groups - 1):
        combine(g)
    finish_first()
    combine(groups - 1)
    combine(0)

    swap.wait_send()
    own.wait_send()
    wait_bytes(proj.at[core, pl.ds(0, 1), :, pl.ds(0, N - 1)], ring1_send)
    wait_bytes(proj.at[core, pl.ds(0, N - 1)], ring2_send)
    wait_bytes(proj.at[core, pl.ds(0, 1), :, pl.ds(0, N - 1)], copy_send.at[0])
    wait_bytes(proj.at[core, pl.ds(0, N - 1)], copy_send.at[1])
    wait_bytes(outbox.at[pl.ds(0, experts - 1)], out_send)
    wait_bytes(inbox.at[:, 0], fwd_send)
    wait_bytes(others, half_send)
    wait_bytes(outbox.at[pl.ds(0, experts - 1)], home_send)


def on_device(tokens, context, out_proj, norm_gain, router, expert_ids, w_gate_up, w_down):
    T, D = tokens.shape
    E, F = lax.axis_size("expert"), lax.axis_size("fsdp")
    Y, pairs = E // 2, F // 2
    experts = E * pairs
    cap = 5 * T // (2 * experts)
    J = D // 128
    R = out_proj.shape[0]
    half_units = w_down.shape[1]
    slots = experts * cap
    chunk = E // 4
    rows = chunk * 2 * pairs * cap
    N = F
    vmem, dma = pltpu.VMEM, pltpu.SemaphoreType.DMA
    any_space = pl.BlockSpec(memory_space=pl.ANY)
    in_vmem = pl.BlockSpec(memory_space=pltpu.VMEM)
    return pl.pallas_call(
        functools.partial(block_kernel, (E, F, cap, chunk)),
        out_shape=pltpu.VMEM((T, D), bf16),
        in_specs=[any_space, any_space, any_space, in_vmem, in_vmem, in_vmem, any_space, any_space],
        out_specs=in_vmem,
        scratch_shapes=[
            vmem((2, Y, 2, F, R, D // 2), bf16),
            vmem((T, D), bf16), vmem((T, D), bf16), vmem((T, D), bf16), vmem((T, D), bf16),
            vmem((2, half_units, D), bf16), vmem((half_units, D), bf16),
            vmem((slots, T), bf16), vmem((E // chunk, 2 * T, chunk * pairs * cap), bf16),
            vmem((T, experts), f32), vmem((T, experts), f32), vmem((T, D), f32),
            vmem((max(slots, rows), J, 128), f32),
            vmem((experts, cap, J, 128), bf16),
            vmem((E, 2, pairs, cap, J, 128), bf16),
            vmem((rows, D), bf16), vmem((rows, half_units), bf16),
            vmem((E, 2, pairs, cap, J, 128), bf16),
            vmem((E, pairs, cap, J, 128), bf16),
            vmem((E, pairs, cap, J, 128), bf16),
            dma((6,)), dma((4,)), dma, dma((N,)), dma, dma((N * N,)), dma((2,)), dma((2,)),
            dma, dma((E,)), dma, dma((E,)), dma, dma((E,)), dma, dma((E,)),
        ],
        compiler_params=pltpu.CompilerParams(
            collective_id=0, has_side_effects=True, vmem_limit_bytes=56 * 1024 * 1024
        ),
        name="block",
    )(
        tokens, context, out_proj, norm_gain.reshape(1, D), router.T, expert_ids.T, w_gate_up, w_down
    )


def solution(mesh):
    return jax.shard_map(
        on_device,
        mesh=mesh,
        in_specs=(
            P(("sweep", "expert", "fsdp"), None),
            P(("sweep", "expert", "fsdp"), None),
            P(("sweep", "expert", "fsdp"), None),
            P("sweep"),
            P("sweep", None),
            P(("sweep", "expert", "fsdp"), None),
            P(("sweep", "expert", "fsdp"), None, None, None),
            P(("sweep", "expert", "fsdp"), None, None),
        ),
        out_specs=P(("sweep", "expert", "fsdp"), None),
        check_vma=False,
    )
```

```python
import functools

import jax
import jax.numpy as jnp
from jax import lax
from jax.experimental import pallas as pl
from jax.experimental.pallas import tpu as pltpu
from jax.sharding import PartitionSpec as P

eps_norm = 1e-05
MESH = pl.DeviceIdType.MESH
f32, bf16 = jnp.float32, jnp.bfloat16


def block_kernel(
    dims,
    tokens_hbm, context_hbm, shard_hbm, gain_ref, router_ref, ids_ref, gate_up_hbm, down_hbm,
    out_ref,
    proj, tok, ctx, resid, normed, gate_up, down,
    slot_rows, picks, mask0, mask1, total,
    wide, outbox, inbox, rows2d, hidden, halves, others, finished,
    load_sem, pair_sem, ring1_send, ring1_recv, ring2_send, ring2_recv, copy_send, copy_recv,
    out_send, out_recv, fwd_send, fwd_recv, half_send, half_recv, home_send, home_recv,
):
    E, F, cap, chunk = dims
    T, D = out_ref.shape
    J = D // 128
    Y, pairs = E // 2, F // 2
    experts = E * pairs
    slots = experts * cap
    rem, div = lax.rem, lax.div

    c = lax.axis_index("expert")
    x = lax.axis_index("fsdp")
    y, core = div(c, 2), rem(c, 2)
    par = rem(x, 2)
    tau = 1 - 2 * par

    def dev(cc, xx):
        return {"expert": cc, "fsdp": xx}

    def wait_bytes(ref, sem):
        pltpu.make_async_copy(ref, ref, sem).wait()

    Dh = D // 2
    loads = [
        pltpu.make_async_copy(shard_hbm.at[:, h * Dh:(h + 1) * Dh], proj.at[h, y, core, x], load_sem.at[h])
        for h in range(2)
    ]
    loads.append(pltpu.make_async_copy(context_hbm, ctx, load_sem.at[2]))
    loads.append(pltpu.make_async_copy(tokens_hbm, tok, load_sem.at[3]))
    loads.append(pltpu.make_async_copy(gate_up_hbm.at[0], gate_up, load_sem.at[4]))
    loads.append(pltpu.make_async_copy(down_hbm.at[0], down, load_sem.at[5]))
    for load in loads:
        load.start()

    N = F
    partner_core = dev(c + 1 - 2 * core, x)
    first = [partner_core]
    first += [dev(c, rem(x + n, F)) for n in (1, F - 1)] + [dev(rem(c + n, E), x) for n in (2, E - 2)]
    barrier = pltpu.get_barrier_semaphore()
    for other in first:
        pl.semaphore_signal(barrier, inc=1, device_id=other, device_id_type=MESH)
    pl.semaphore_wait(barrier, len(first))

    loads[0].wait()
    loads[1].wait()
    swap = pltpu.make_async_remote_copy(
        src_ref=proj.at[1 - core, y, core, x], dst_ref=proj.at[1 - core, y, core, x],
        send_sem=pair_sem.at[0], recv_sem=pair_sem.at[1], device_id=partner_core, device_id_type=MESH,
    )
    swap.start()
    own = pltpu.make_async_remote_copy(
        src_ref=proj.at[core, y, core, x], dst_ref=proj.at[core, y, core, x],
        send_sem=pair_sem.at[2], recv_sem=pair_sem.at[3], device_id=partner_core, device_id_type=MESH,
    )
    own.start()
    swap.wait_recv()

    pos1 = x * (1 - core) + y * core
    pos2 = y * (1 - core) + x * core

    def piece(p1, p2):
        return proj.at[core, p2 * (1 - core) + p1 * core, :, p1 * (1 - core) + p2 * core]

    def at(p1, p2):
        return dev(2 * (p2 * (1 - core) + p1 * core) + core, p1 * (1 - core) + p2 * core)

    def ring1(way, step, p1):
        sign = 1 - 2 * way
        ref = piece(p1, pos2)
        return pltpu.make_async_remote_copy(
            src_ref=ref, dst_ref=ref, send_sem=ring1_send, recv_sem=ring1_recv.at[way * (N // 2) + step],
            device_id=at(rem(pos1 + sign + N, N), pos2), device_id_type=MESH,
        )

    def ring2(way, step, p1, p2, o):
        sign = 1 - 2 * way
        ref = piece(p1, p2)
        return pltpu.make_async_remote_copy(
            src_ref=ref, dst_ref=ref, send_sem=ring2_send,
            recv_sem=ring2_recv.at[(way * (N // 2) + step) * N + o],
            device_id=at(pos1, rem(pos2 + sign + N, N)), device_id_type=MESH,
        )

    def to_partner(p1, p2, which):
        ref = piece(p1, p2)
        return pltpu.make_async_remote_copy(
            src_ref=ref, dst_ref=ref, send_sem=copy_send.at[which], recv_sem=copy_recv.at[which],
            device_id=partner_core, device_id_type=MESH,
        )

    ring2(0, 0, pos1, pos2, 0).start()
    ring2(1, 0, pos1, pos2, 0).start()
    for way in range(2):
        ring1(way, 0, pos1).start()

    ids = ids_ref[...]
    expert_row = lax.broadcasted_iota(jnp.int32, (experts, T), 0)
    one0 = (expert_row == ids[0:1, :]).astype(f32)
    one1 = (expert_row == ids[1:2, :]).astype(f32)
    earlier = (
        lax.broadcasted_iota(jnp.int32, (T, T), 0) < lax.broadcasted_iota(jnp.int32, (T, T), 1)
    ).astype(bf16)
    before = jnp.dot((one0 + one1).astype(bf16), earlier, preferred_element_type=f32)
    place0 = jnp.sum(before * one0, axis=0, keepdims=True).astype(jnp.int32)
    place1 = jnp.sum(before * one1, axis=0, keepdims=True).astype(jnp.int32)
    slot_row = lax.broadcasted_iota(jnp.int32, (slots, T), 0)
    sel0 = (slot_row == ids[0:1, :] * cap + place0).astype(f32)
    sel1 = (slot_row == ids[1:2, :] * cap + place1).astype(f32)
    slot_rows[...] = (sel0 + sel1).astype(bf16)
    expert = lax.broadcasted_iota(jnp.int32, (experts, 1), 0)
    ahead = jnp.right_shift(expert, pairs.bit_length() - 1) - c
    ahead = jnp.where(ahead < 0, ahead + E, ahead)
    turn_of = jnp.where(ahead > E // 2, 2 * (E - ahead), 2 * ahead - jnp.minimum(ahead, 1))
    start = (turn_of * (pairs * cap) + jnp.bitwise_and(expert, pairs - 1) * cap).astype(f32)
    home0 = jnp.sum((before + start) * one0, axis=0, keepdims=True).astype(jnp.int32)
    home1 = jnp.sum((before + start) * one1, axis=0, keepdims=True).astype(jnp.int32)
    part = chunk * pairs * cap
    for n, home in enumerate((home0, home1)):
        chosen = jnp.transpose((slot_row == home).astype(f32)).astype(bf16)
        for g in range(E // chunk):
            picks[g, n * T:(n + 1) * T, :] = chosen[:, g * part:(g + 1) * part]
    mask0[...] = jnp.transpose(one0)
    mask1[...] = jnp.transpose(one1)

    def pass_on(o, step, last):
        p1 = rem(pos1 + (o // 2 if o % 2 == 0 else N - (o + 1) // 2), N)
        for way in range(2):
            hops = N // 2 if way == o % 2 else N // 2 - 1
            if step > hops or last != (step == hops):
                continue
            p2 = rem(pos2 + (N - step if way == 0 else step), N)
            ring2(way, step - 1, p1, p2, o).wait_recv()
            if step < hops:
                ring2(way, step, p1, p2, o).start()
            to_partner(p1, p2, 1).start()

    for slot in range(1, N + 1 + 1):
        if slot <= N // 2:
            for way in range(2):
                if way == 1 and slot == N // 2:
                    continue
                p1 = rem(pos1 + (N - slot if way == 0 else slot), N)
                o = 2 * slot - 1 + way
                ring1(way, slot - 1, p1).wait_recv()
                if slot < N // 2 - way:
                    ring1(way, slot, p1).start()
                ring2(0, 0, p1, pos2, o).start()
                ring2(1, 0, p1, pos2, o).start()
                to_partner(p1, pos2, 0).start()
        for o in range(N - 1, -1, -1):
            step = slot - (o + 1) // 2
            if 1 <= step < N // 2:
                pass_on(o, step, False)
        for o in range(N):
            step = slot - 1 - (o + 1) // 2
            if N // 2 - 1 <= step <= N // 2:
                pass_on(o, step, True)

    loads[2].wait()
    loads[3].wait()
    wide_cols = 512 if D >= 2048 else 128
    squares = jnp.zeros((T, 1), f32)
    for turn in range(2):
        h = core if turn == 0 else 1 - core
        if turn == 1:
            own.wait_recv()
            wait_bytes(proj.at[1 - core, pl.ds(0, 1), :, pl.ds(0, N - 1)], copy_recv.at[0])
            wait_bytes(proj.at[1 - core, pl.ds(0, N - 1)], copy_recv.at[1])
        for off in range(0, Dh, wide_cols):
            weights = proj[h, :, :, :, :, off:off + wide_cols].reshape(D, wide_cols)
            attended = jnp.dot(ctx[...], weights, preferred_element_type=f32)
            cols = pl.ds(pl.multiple_of(h * Dh + off, wide_cols), wide_cols)
            r = (tok[:, cols].astype(f32) + attended).astype(bf16)
            resid[:, cols] = r
            r = r.astype(f32)
            squares = squares + jnp.sum(r * r, axis=1, keepdims=True)
    inv_rms = lax.rsqrt(squares * (1.0 / D) + eps_norm)
    for n in range(D // wide_cols):
        cols = slice(n * wide_cols, (n + 1) * wide_cols)
        normed[:, cols] = (resid[:, cols].astype(f32) * inv_rms * gain_ref[:, cols]).astype(bf16)

    for jj in range(J // 2):
        cols = slice(256 * jj, 256 * jj + 256)
        got = jnp.dot(slot_rows[...], normed[:, cols], preferred_element_type=f32)
        wide[0:slots, 2 * jj, :] = got[:, :128]
        wide[0:slots, 2 * jj + 1, :] = got[:, 128:]
    eb = 4

    def narrow(n, carry):
        block = wide[pl.ds(n * eb * cap, eb * cap)].astype(bf16)
        outbox[pl.ds(n * eb, eb)] = block.reshape(eb, cap, J, 128)
        return carry

    lax.fori_loop(0, experts // eb, narrow, 0)

    def shift(k):
        return div(k + 1, 2) * rem(k, 2) + rem(E - div(k, 2), E) * (1 - rem(k, 2))

    def near(i):
        return rem(x + tau * (i if i % 2 == 0 else -i) + F, F)

    def send_slot(k, i):
        to_c, to_x = rem(c + shift(k), E), near(i)
        return pltpu.make_async_remote_copy(
            src_ref=outbox.at[pairs * to_c + div(to_x, 2)], dst_ref=inbox.at[c, rem(to_x, 2), i],
            send_sem=out_send, recv_sem=out_recv.at[k], device_id=dev(to_c, to_x), device_id_type=MESH,
        )

    for i in range(pairs - 1, 0, -1):
        send_slot(0, i).start()
    inbox[c, par, 0] = outbox[pairs * c + div(x, 2)]

    def send_round(k, carry):
        for i in range(pairs - 1, -1, -1):
            send_slot(k, i).start()
        return carry

    lax.fori_loop(1, E, send_round, 0)

    logits = lax.dot_general(
        normed[...], router_ref[...], (((1,), (1,)), ((), ())), preferred_element_type=f32
    )
    score0 = 1.0 / (1.0 + jnp.exp(-jnp.sum(logits * mask0[...], axis=1, keepdims=True)))
    score1 = 1.0 / (1.0 + jnp.exp(-jnp.sum(logits * mask1[...], axis=1, keepdims=True)))
    gate0 = score0 / (score0 + score1)
    gate1 = score1 / (score0 + score1)

    partner = dev(c, x + tau)

    def source(k):
        return rem(c + E - shift(k), E)

    def forward(k):
        ref = inbox.at[source(k), par]
        return pltpu.make_async_remote_copy(
            src_ref=ref, dst_ref=ref, send_sem=fwd_send, recv_sem=fwd_recv.at[k],
            device_id=partner, device_id_type=MESH,
        )

    def pump(g):
        def one(kk, carry):
            k = g * chunk + kk
            wait_bytes(inbox.at[0, 0], out_recv.at[k])
            forward(k).start()
            return carry

        lax.fori_loop(0, chunk, one, 0)

    def pump_first():
        wait_bytes(inbox.at[0, 0, pl.ds(0, pairs - 1)], out_recv.at[0])
        forward(0).start()

        def one(k, carry):
            wait_bytes(inbox.at[0, 0], out_recv.at[k])
            forward(k).start()
            return carry

        lax.fori_loop(1, chunk, one, 0)

    per = 2 * pairs * cap
    rows = chunk * per

    def half_back(k):
        src = source(k)
        return pltpu.make_async_remote_copy(
            src_ref=halves.at[src, 1 - par], dst_ref=others.at[src], send_sem=half_send, recv_sem=half_recv.at[k],
            device_id=partner, device_id_type=MESH,
        )

    def experts_on(g):
        def take(kk, carry):
            k = g * chunk + kk
            wait_bytes(inbox.at[0, 0], fwd_recv.at[k])
            block = inbox[source(k)].reshape(per, J, 128)
            wide[pl.ds(kk * per, per)] = block.astype(f32)
            return carry

        lax.fori_loop(0, chunk, take, 0)
        for jj in range(J // 2):
            both = jnp.concatenate([wide[0:rows, 2 * jj, :], wide[0:rows, 2 * jj + 1, :]], axis=1)
            rows2d[:, 256 * jj:256 * jj + 256] = both.astype(bf16)
        over_last = (((1,), (1,)), ((), ()))
        gate = lax.dot_general(rows2d[...], gate_up[0], over_last, preferred_element_type=f32)
        up = lax.dot_general(rows2d[...], gate_up[1], over_last, preferred_element_type=f32)
        hidden[...] = (gate / (1.0 + jnp.exp(-gate)) * up).astype(bf16)
        for jj in range(J // 2):
            got = jnp.dot(hidden[...], down[:, 256 * jj:256 * jj + 256], preferred_element_type=f32)
            wide[0:rows, 2 * jj, :] = got[:, :128]
            wide[0:rows, 2 * jj + 1, :] = got[:, 128:]

        def give(kk, carry):
            k = g * chunk + kk
            block = wide[pl.ds(kk * per, per)].astype(bf16)
            halves[source(k)] = block.reshape(2, pairs, cap, J, 128)
            if g > 0:
                half_back(k).start()
            return carry

        lax.fori_loop(0, chunk, give, 0)

    mine = div(x, 2)

    def send_home(k, i):
        src = source(k)
        return pltpu.make_async_remote_copy(
            src_ref=halves.at[src, par, i], dst_ref=finished.at[k, mine], send_sem=home_send,
            recv_sem=home_recv.at[k],
            device_id=dev(src, rem(x - tau * i + F, F)), device_id_type=MESH,
        )

    def add_halves(k):
        src = source(k)
        wait_bytes(others.at[0], half_recv.at[k])
        both = halves[src, par].astype(f32) + others[src].astype(f32)
        halves[src, par] = both.astype(bf16)

    def finish(g):
        def one(kk, carry):
            k = g * chunk + kk
            add_halves(k)
            for i in range(pairs - 1, -1, -1):
                send_home(k, i).start()
            return carry

        lax.fori_loop(0, chunk, one, 0)

    def finish_first():
        add_halves(0)
        for i in range(pairs - 1, 0, -1):
            send_home(0, i).start()
        finished[0, mine] = halves[c, par, 0]

        def one(k, carry):
            add_halves(k)
            for i in range(pairs - 1, -1, -1):
                send_home(k, i).start()
            return carry

        lax.fori_loop(1, chunk, one, 0)

    loads[4].wait()
    loads[5].wait()
    groups = E // chunk

    def widen(k):
        wide[pl.ds(rem(k, chunk) * pairs * cap, pairs * cap)] = finished[k].reshape(pairs * cap, J, 128).astype(f32)

    def arrived(k, carry):
        wait_bytes(finished.at[0], home_recv.at[k])
        widen(k)
        return carry

    def combine(g):
        if g == 0:
            wait_bytes(finished.at[0, pl.ds(0, pairs - 1)], home_recv.at[0])
            widen(0)
        lax.fori_loop(max(1, g * chunk), (g + 1) * chunk, arrived, 0)
        for jj in range(J // 2):
            cols = slice(256 * jj, 256 * jj + 256)
            got = jnp.concatenate([wide[0:part, 2 * jj, :], wide[0:part, 2 * jj + 1, :]], axis=1).astype(bf16)
            picked = jnp.dot(picks[g], got, preferred_element_type=f32)
            so_far = resid[:, cols].astype(f32) if g == 1 else total[:, cols]
            so_far = so_far + gate0 * picked[:T] + gate1 * picked[T:]
            if g < groups - 1:
                total[:, cols] = so_far
            else:
                out_ref[:, cols] = so_far.astype(bf16)


    def go_back(k, carry):
        half_back(k).start()
        return carry

    pump_first()
    for g in range(1, groups):
        pump(g)
    experts_on(0)
    experts_on(1)
    for g in range(2, groups):
        experts_on(g)
        if g == groups - 1:
            lax.fori_loop(0, chunk, go_back, 0)
        finish(g - 1)

    finish(groups - 1)
    for g in range(1, groups - 1):
        combine(g)
    finish_first()
    combine(0)
    combine(groups - 1)

    swap.wait_send()
    own.wait_send()
    wait_bytes(proj.at[core, pl.ds(0, 1), :, pl.ds(0, N - 1)], ring1_send)
    wait_bytes(proj.at[core, pl.ds(0, N - 1)], ring2_send)
    wait_bytes(proj.at[core, pl.ds(0, 1), :, pl.ds(0, N - 1)], copy_send.at[0])
    wait_bytes(proj.at[core, pl.ds(0, N - 1)], copy_send.at[1])
    wait_bytes(outbox.at[pl.ds(0, experts - 1)], out_send)
    wait_bytes(inbox.at[:, 0], fwd_send)
    wait_bytes(others, half_send)
    wait_bytes(outbox.at[pl.ds(0, experts - 1)], home_send)


def on_device(tokens, context, out_proj, norm_gain, router, expert_ids, w_gate_up, w_down):
    T, D = tokens.shape
    E, F = lax.axis_size("expert"), lax.axis_size("fsdp")
    Y, pairs = E // 2, F // 2
    experts = E * pairs
    cap = 5 * T // (2 * experts)
    J = D // 128
    R = out_proj.shape[0]
    half_units = w_down.shape[1]
    slots = experts * cap
    chunk = E // 4
    rows = chunk * 2 * pairs * cap
    N = F
    vmem, dma = pltpu.VMEM, pltpu.SemaphoreType.DMA
    any_space = pl.BlockSpec(memory_space=pl.ANY)
    in_vmem = pl.BlockSpec(memory_space=pltpu.VMEM)
    return pl.pallas_call(
        functools.partial(block_kernel, (E, F, cap, chunk)),
        out_shape=pltpu.VMEM((T, D), bf16),
        in_specs=[any_space, any_space, any_space, in_vmem, in_vmem, in_vmem, any_space, any_space],
        out_specs=in_vmem,
        scratch_shapes=[
            vmem((2, Y, 2, F, R, D // 2), bf16),
            vmem((T, D), bf16), vmem((T, D), bf16), vmem((T, D), bf16), vmem((T, D), bf16),
            vmem((2, half_units, D), bf16), vmem((half_units, D), bf16),
            vmem((slots, T), bf16), vmem((E // chunk, 2 * T, chunk * pairs * cap), bf16),
            vmem((T, experts), f32), vmem((T, experts), f32), vmem((T, D), f32),
            vmem((max(slots, rows), J, 128), f32),
            vmem((experts, cap, J, 128), bf16),
            vmem((E, 2, pairs, cap, J, 128), bf16),
            vmem((rows, D), bf16), vmem((rows, half_units), bf16),
            vmem((E, 2, pairs, cap, J, 128), bf16),
            vmem((E, pairs, cap, J, 128), bf16),
            vmem((E, pairs, cap, J, 128), bf16),
            dma((6,)), dma((4,)), dma, dma((N,)), dma, dma((N * N,)), dma((2,)), dma((2,)),
            dma, dma((E,)), dma, dma((E,)), dma, dma((E,)), dma, dma((E,)),
        ],
        compiler_params=pltpu.CompilerParams(
            collective_id=0, has_side_effects=True, vmem_limit_bytes=56 * 1024 * 1024
        ),
        name="block",
    )(
        tokens, context, out_proj, norm_gain.reshape(1, D), router.T, expert_ids.T, w_gate_up, w_down
    )


def solution(mesh):
    return jax.shard_map(
        on_device,
        mesh=mesh,
        in_specs=(
            P(("sweep", "expert", "fsdp"), None),
            P(("sweep", "expert", "fsdp"), None),
            P(("sweep", "expert", "fsdp"), None),
            P("sweep"),
            P("sweep", None),
            P(("sweep", "expert", "fsdp"), None),
            P(("sweep", "expert", "fsdp"), None, None, None),
            P(("sweep", "expert", "fsdp"), None, None),
        ),
        out_specs=P(("sweep", "expert", "fsdp"), None),
        check_vma=False,
    )
```
